32 devices in a mesh: seq: 8 (over y, x, core), head: 4 (over z).
Axes of the slice: x: 2, y: 2, z: 4, core: 2. Of those that a mesh axis runs over, the one named last changes fastest.
Arguments:
- queries: bfloat16 [2048, 16384], P('seq', 'head'), may hold values from -6 to 6
- keys: bfloat16 [2048, 1024], P('seq', 'head'), may hold values from -6 to 6
- values: bfloat16 [2048, 1024], P('seq', 'head'), may hold values from -6 to 6
- teacher: bfloat16 [2048, 16384], P('seq', 'head'), may hold values from -17 to 17
- map_q: bfloat16 [128, 128, 64], P('head'), may hold values from -0.5 to 0.5
- map_k: bfloat16 [128, 128, 64], P('head'), may hold values from -0.5 to 0.5
Outputs:
- grad_map_q: float32 [128, 128, 64], P('head', 'seq')
- grad_map_k: float32 [128, 128, 64], P('head', 'seq')
The draws below stay inside these ranges and needn't reach their ends.
All inputs are finite; a program needn't handle non-finite values.
Results may differ from the reference program's by a relative error of at most 0.0003.
Values sent between devices are 32-bit elements; how exact they have to be, the bound alone decides.
No kernel may reach another device: no remote copies, remote signals or barrier semaphores. Data moves between devices by JAX's collectives and lax.ppermute only.
A program may use at most 128 MiB of HBM per device.

```python
import jax
import jax.numpy as jnp
from jax import lax

HEADS = 128
KV_HEADS = 8
DH = 128
FH = 64
BLOCK = 256
SEQ = 2048


def draw_teacher(key, part):
    row_count = SEQ
    col_count = HEADS * DH
    head_pos = (jnp.arange(col_count, dtype=jnp.int32) // DH).astype(jnp.float32)
    rising = 1.0 + 2.0 * head_pos / max(HEADS - 1, 1)
    base = jax.random.truncated_normal(jax.random.fold_in(key, 5), -4.0, 4.0, (row_count, col_count), jnp.float32)
    return (base * rising[None, :]).astype(jnp.bfloat16)


def level_of(stream_key, extent, split, smallest, top_value):
    gain, own = 1.0, jax.random.fold_in(stream_key, 6)
    for dim, blocks in split:
        draws = jnp.exp(jax.random.uniform(jax.random.fold_in(own, dim), (blocks,), jnp.float32, smallest / len(split), top_value / len(split)))
        gain = gain * jnp.repeat(draws, extent[dim] // blocks).reshape([-1 if axis == dim else 1 for axis in range(len(extent))])
    return gain


def bell_draw(stream_key, extent, scale, bound, pieces=(), kind=jnp.bfloat16):
    values = scale * jax.random.normal(stream_key, extent, jnp.float32)
    if pieces:
        values = values * level_of(stream_key, extent, pieces, -0.22, 0.18)
    return jnp.clip(values, -bound, bound).astype(kind)


def setup_inputs(seed: int = 0) -> dict:
    key_list = jax.random.split(jax.random.key(seed), 7)
    return {
        "queries": bell_draw(key_list[0], (SEQ, HEADS * DH), 1.0, 6.0, ((0, 8), (1, 4))),
        "keys": bell_draw(key_list[1], (SEQ, KV_HEADS * DH), 1.0, 6.0, ((0, 8), (1, 4))),
        "values": bell_draw(key_list[2], (SEQ, KV_HEADS * DH), 1.0, 6.0, ((0, 8), (1, 4))),
        "teacher": draw_teacher(jax.random.fold_in(key_list[6], 71), 0),
        "map_q": bell_draw(key_list[4], (HEADS, DH, FH), DH ** -0.5, 0.5, ((0, 4),)),
        "map_k": bell_draw(key_list[5], (HEADS, DH, FH), DH ** -0.5, 0.5, ((0, 4),)),
    }


exact_mode = lax.Precision.HIGHEST

def features(inputs, weight):
    logits = jnp.dot(inputs.astype(jnp.float32), weight, precision=exact_mode)
    positive = jnp.exp(logits)
    negative = jnp.exp(-logits)
    return jnp.concatenate([positive / lax.optimization_barrier(jnp.sum(positive, -1, keepdims=True)), negative / lax.optimization_barrier(jnp.sum(negative, -1, keepdims=True))], -1)

def head_loss(w_query, w_key, queries, keys, values, teacher, power):
    query_feat = features(queries, w_query)
    key_feat = features(keys, w_key)
    block_count = queries.shape[0] // BLOCK
    causal = jnp.tril(jnp.ones((BLOCK, BLOCK), jnp.float32))

    def step(carried, blocks):
        kv_state, key_total = carried
        q_blk, k_blk, v_blk, t_blk, p_blk = blocks
        scores = jnp.dot(q_blk, k_blk.T, precision=exact_mode) * causal
        numerator = jnp.dot(q_blk, kv_state, precision=exact_mode) + jnp.dot(scores, v_blk, precision=exact_mode)
        denominator = jnp.dot(q_blk, key_total, precision=exact_mode) + lax.optimization_barrier(jnp.sum(scores, -1))
        student = numerator / denominator[:, None]
        error = student - t_blk
        partial_loss = 0.5 * jnp.sum(error * error / p_blk[:, None])
        new_state = kv_state + jnp.dot(k_blk.T, v_blk, precision=exact_mode)
        return ((new_state, key_total + lax.optimization_barrier(jnp.sum(k_blk, 0))), partial_loss)
    feat_width = query_feat.shape[1]
    start = (jnp.zeros((feat_width, DH), jnp.float32), jnp.zeros((feat_width,), jnp.float32))
    blocks = (query_feat.reshape(block_count, BLOCK, feat_width), key_feat.reshape(block_count, BLOCK, feat_width), values.astype(jnp.float32).reshape(block_count, BLOCK, DH), teacher.astype(jnp.float32).reshape(block_count, BLOCK, DH), power.reshape(block_count, BLOCK))
    _, partials = lax.scan(step, start, blocks)
    return jnp.sum(partials)

def reference(queries, keys, values, teacher, map_q, map_k):
    power = lax.optimization_barrier(jnp.sum(jnp.square(teacher.astype(jnp.float32)), axis=1)) / (HEADS * DH) + 1e-05
    group_size = HEADS // KV_HEADS

    def one_head(head_idx):
        offset = (head_idx * DH).astype(jnp.int32)
        shared = (head_idx // group_size * DH).astype(jnp.int32)

        def take_head(source):
            return lax.dynamic_slice_in_dim(source, offset, DH, 1)

        def take_shared(source):
            return lax.dynamic_slice_in_dim(source, shared, DH, 1)
        return jax.grad(head_loss, argnums=(0, 1))(map_q[head_idx].astype(jnp.float32), map_k[head_idx].astype(jnp.float32), take_head(queries), take_shared(keys), take_shared(values), take_head(teacher), power)
    grad_q, grad_k = lax.map(one_head, jnp.arange(HEADS, dtype=jnp.int32))
    return (grad_q, grad_k)
```

```python
import functools

import jax
import jax.numpy as jnp
from jax import lax
from jax.experimental import pallas as pl
from jax.experimental.pallas import tpu as pltpu
from jax.sharding import PartitionSpec as P

F32, BF16 = jnp.float32, jnp.bfloat16
LANES = 128
ROWS = 16
STEP_A = 2
STEP_B = 4
PARTS = (1, 1)
VMEM_LIMIT = 60 * 1024 * 1024


def split(x):
    high = x.astype(BF16)
    return high, (x - high.astype(F32)).astype(BF16)


def mm(a, b):
    return jnp.dot(a, b, preferred_element_type=F32)


def mm_nt(a, b):
    return lax.dot_general(a, b, (((1,), (1,)), ((), ())), preferred_element_type=F32)


def cat(parts, axis):
    return jnp.concatenate(parts, axis)


def features(logits):
    up, down = jnp.exp(logits), jnp.exp(-logits)
    up = up * (1.0 / jnp.sum(up, 0, keepdims=True))
    down = down * (1.0 / jnp.sum(down, 0, keepdims=True))
    return cat([up, down], 0)


def features_back(feat, grad):
    half = feat.shape[0] // 2
    prod = feat * grad
    up, down = prod[:half], prod[half:]
    up = up - feat[:half] * jnp.sum(up, 0, keepdims=True)
    down = down - feat[half:] * jnp.sum(down, 0, keepdims=True)
    return up - down


def causal_mask(size):
    row = lax.broadcasted_iota(jnp.int32, (size, size), 0)
    col = lax.broadcasted_iota(jnp.int32, (size, size), 1)
    return row <= col


def with_ones(v):
    return cat([v, jnp.ones_like(v)], 1)


def local_kernel(pair, block, width, half, pos_ref, *refs):
    refs = list(refs)
    q_own = refs.pop(0)
    q_got = refs.pop(0) if pair > 1 else None
    wq, wk, kv = refs[:3]
    q_out, qh_out, ql_out, kh_out, kl_out, num_out, state_out = refs[3:10]
    k_nat, v_aug, v_tr = refs[10:]
    heads = wq.shape[0]
    tokens = pair * block

    @pl.when(pl.program_id(0) == 0)
    def _():
        k_nat[...] = kv[:, :width].astype(BF16)
        v = kv[:, width:]
        v_aug[...] = with_ones(v).astype(BF16)
        v_tr[:width] = v.T.astype(BF16)
        v_tr[width:] = jnp.ones((ROWS, tokens), BF16)

    mask = causal_mask(block)
    k_logits = mm_nt(wk[...].reshape(heads * half, width), k_nat[...])
    for h in range(heads):
        cols = slice(h * width, (h + 1) * width)
        if pair > 1:
            place = pos_ref[0]
            q_out[h, pl.ds(pl.multiple_of(place * block, block), block)] = q_own[:, cols]
            q_out[h, pl.ds(pl.multiple_of((1 - place) * block, block), block)] = q_got[
                :, cols
            ].astype(BF16)
        else:
            q_out[h] = q_own[:, cols]
        qh, ql = split(features(mm_nt(wq[h], q_out[h])))
        kh, kl = split(features(k_logits[h * half : (h + 1) * half]))
        qh_out[h] = qh
        ql_out[h] = ql
        kh_out[h] = kh
        kl_out[h] = kl
        for b in range(pair):
            at = slice(b * block, (b + 1) * block)
            kth, ktl = kh[:, at].T, kl[:, at].T
            scores = mm(cat([kth, kth, ktl], 1), cat([qh[:, at], ql[:, at], qh[:, at]], 0))
            sh, sl = split(jnp.where(mask, scores, 0.0))
            vt = v_tr[:, at]
            num_out[h, b] = mm(cat([vt, vt], 1), cat([sh, sl], 0))
        if pair > 1:
            va = v_aug[:block]
            state_out[h] = mm(cat([kh[:, :block], kl[:, :block]], 1), cat([va, va], 0))
        else:
            state_out[h] = jnp.zeros(state_out.shape[1:], F32)


def global_kernel(pair, units, block, width, half, pos_ref, *refs):
    refs = list(refs)
    q, qh_in, ql_in, kh_in, kl_in, num_in, state_in, wk, t_own = refs[:9]
    refs = refs[9:]
    t_got = refs.pop(0) if pair > 1 else None
    inv_power, kv = refs[:2]
    out = refs[2]
    k_nat, v_aug, v_tr, feat_old, state, grad_high, grad_low, grad_k, gsum = refs[3:]
    heads = wk.shape[0]
    tokens = pair * block
    place, unit = pos_ref[0], pos_ref[1]

    @pl.when(pl.program_id(0) == 0)
    def _():
        for o in range(units):
            k_nat[o] = kv[o, :, :width].astype(BF16)
            v = kv[o, :, width:]
            v_aug[o] = with_ones(v).astype(BF16)
            v_tr[o, :width] = v.T.astype(BF16)
            v_tr[o, width:] = jnp.ones((width, tokens), BF16)
        grad_high[...] = jnp.zeros_like(grad_high)
        grad_low[...] = jnp.zeros_like(grad_low)

    wk_all = wk[...].reshape(heads * half, width)
    state[...] = jnp.zeros_like(state)

    def ahead(u, carry):
        o = unit ^ u
        logits = mm_nt(wk_all, k_nat[o])
        highs, lows = [], []
        for h in range(heads):
            feat = features(logits[h * half : (h + 1) * half])
            feat_old[u, h] = feat
            fh, fl = split(feat)
            highs.append(fh)
            lows.append(fl)
        va = v_aug[o]
        state[...] += mm(cat([cat(highs, 0), cat(lows, 0)], 1), cat([va, va], 0))
        return carry

    lax.fori_loop(0, unit, ahead, 0)

    mask = causal_mask(block)
    for h in range(heads):
        total_state = state[h * 2 * half : (h + 1) * 2 * half]
        grad_q = jnp.zeros((half, width), F32)
        sums = []
        key_grads = []
        for b in range(pair):
            at = slice(b * block, (b + 1) * block)
            if b == 1:
                total_state = total_state + state_in[h]
            sth, stl = split(total_state)
            turned = total_state.T[: width + ROWS]
            tth, ttl = split(turned)
            qh, ql = qh_in[h, :, at], ql_in[h, :, at]
            kh, kl = kh_in[h, :, at], kl_in[h, :, at]
            numer = num_in[h, b] + mm(cat([tth, tth, ttl], 1), cat([qh, ql, qh], 0))
            inv = 1.0 / numer[width : width + 1]
            student = numer[:width] * inv
            own_t = t_own[:, h * width : (h + 1) * width].astype(F32)
            if pair > 1:
                own_t = jnp.where(place == b, own_t, t_got[:, h * width : (h + 1) * width])
            grad_out = (student - own_t.T) * inv_power[0:1, at]
            gnum = grad_out * inv
            gden = -jnp.sum(grad_out * student, 0, keepdims=True) * inv
            top = lax.broadcasted_iota(jnp.int32, (ROWS, block), 0) == 0
            gh, gl = split(gnum)
            dh, dl = split(jnp.where(top, gden, 0.0))
            grad_high[:width] = gh
            grad_low[:width] = gl
            grad_high[width : width + ROWS] = dh
            grad_low[width : width + ROWS] = dl
            gah, gal = grad_high[...], grad_low[...]
            va = v_aug[0, at]
            back = mm(cat([va, va], 1), cat([gah, gal], 0))
            bh, bl = split(jnp.where(mask, back, 0.0))
            gq = mm(cat([sth, sth, stl], 1), cat([gah, gal, gah], 0)) + mm(
                cat([kh, kh, kl], 1), cat([bh, bl, bh], 0)
            )
            q_feat = qh.astype(F32) + ql.astype(F32)
            lh, ll = split(features_back(q_feat, gq))
            q_nat = q[h, at]
            grad_q = grad_q + mm(cat([lh, ll], 1), cat([q_nat, q_nat], 0))
            small_h, small_l = gah[: width + ROWS], gal[: width + ROWS]
            sums.append(
                mm_nt(cat([small_h, small_h, small_l], 1), cat([qh, ql, qh], 1))
            )
            key_grads.append(mm_nt(cat([qh, qh, ql], 1), cat([bh, bl, bh], 1)))
        grad_kk = jnp.zeros((half, width), F32)
        later = None
        for b in reversed(range(pair)):
            at = slice(b * block, (b + 1) * block)
            gk = key_grads[b]
            if later is not None:
                padded = cat([later, jnp.zeros((width - ROWS, width), F32)], 0).T
                ph, pl_ = split(padded)
                vt = v_tr[0, :, at]
                gk = gk + mm(cat([ph, pl_], 1), cat([vt, vt], 0))
            kh, kl = kh_in[h, :, at], kl_in[h, :, at]
            k_feat = kh.astype(F32) + kl.astype(F32)
            lh, ll = split(features_back(k_feat, gk))
            k_blk = k_nat[0, at]
            grad_kk = grad_kk + mm(cat([lh, ll], 1), cat([k_blk, k_blk], 0))
            later = sums[b] if later is None else later + sums[b]
        padded = cat([later, jnp.zeros((width - ROWS, width), F32)], 0).T
        gsum[h * 2 * half : (h + 1) * 2 * half] = padded
        grad_k[h, :half] = grad_q
        grad_k[h, half:] = grad_kk

    gsh, gsl = split(gsum[...])
    both = cat([gsh, gsl], 1)

    def behind(u, carry):
        o = unit ^ u
        vt = v_tr[o]
        gk = mm(both, cat([vt, vt], 0))
        highs, lows = [], []
        for h in range(heads):
            lh, ll = split(
                features_back(feat_old[u, h], gk[h * 2 * half : (h + 1) * 2 * half])
            )
            highs.append(lh)
            lows.append(ll)
        k_blk = k_nat[o]
        add = mm(cat([cat(highs, 0), cat(lows, 0)], 1), cat([k_blk, k_blk], 0))
        for h in range(heads):
            grad_k[h, half:] += add[h * half : (h + 1) * half]
        return carry

    lax.fori_loop(0, unit, behind, 0)

    share = width // (units * pair)
    for h in range(heads):
        flat = grad_k[h].T
        for u in range(units):
            for r in range(pair):
                slot = (unit ^ u) * pair + (place ^ r)
                start = pl.multiple_of(slot * share, share)
                n = u * pair + r
                out[h, pl.ds(start, share)] = flat[n * share : (n + 1) * share]


def on_device(axis_sizes, queries, keys, values, teacher, map_q, map_k):
    seq_count, head_axis = axis_sizes
    head_count, width, half = map_q.shape
    block = queries.shape[0]
    shared = keys.shape[1] // width
    pair = 2 if shared == 2 and seq_count % 2 == 0 else 1
    units = seq_count // pair
    heads = head_count // pair
    tokens = pair * block
    bits = units.bit_length() - 1
    own = lax.axis_index("seq")
    place, unit = own % pair, own // pair
    pos = jnp.stack([place, unit]).astype(jnp.int32)
    columns = heads * width

    def swap(x, bit):
        return lax.ppermute(x, "seq", [(i, i ^ bit) for i in range(seq_count)])

    def mine(x, size, index):
        return lax.dynamic_slice_in_dim(x, index * size, size, 1)

    def tie(*values):
        return lax.optimization_barrier(values)

    kv = cat([mine(keys, width, place), mine(values, width, place)], 1).astype(F32)
    count = len(PARTS)
    sizes = [heads * n // sum(PARTS) for n in PARTS]
    begins = [sum(sizes[:i]) for i in range(count)]
    first = place == 0
    q_got, t_got = [None] * count, [None] * count
    if pair > 1:
        other = 1 - place
        kv_away = cat([mine(keys, width, other), mine(values, width, other)], 1).astype(F32)
        q_src, kv_away = tie(queries, kv_away)
        kv_got = swap(kv_away, 1)

        def away(source, i):
            start = other * columns + begins[i] * width
            return lax.dynamic_slice_in_dim(source, start, sizes[i] * width, 1).astype(F32)

        q_away = [away(q_src, i) for i in range(count)]
        q_got = [swap(x, 1) for x in q_away]
        t_src, q_last = tie(teacher, q_away[-1])
        t_got = [swap(away(t_src, i), 1) for i in range(count)]
        pieces = [jnp.where(first, kv, kv_got), jnp.where(first, kv_got, kv)]
    else:
        pieces = [kv]
    kv_unit = cat(pieces, 0)

    squares = jnp.sum(jnp.square(teacher.astype(F32)), axis=1)[None]
    others = [
        lax.ppermute(squares, "head", [(i, (i + s) % head_axis) for i in range(head_axis)])
        for s in range(1, head_axis)
    ]

    wq_t, wk_t = jnp.swapaxes(map_q, 1, 2), jnp.swapaxes(map_k, 1, 2)
    two = 2 * half
    whole2 = lambda g, p: (0, 0)
    per_head3 = lambda g, p: (g, 0, 0)
    per_head4 = lambda g, p: (g, 0, 0, 0)
    spec = pl.BlockSpec

    def run_local(i):
        n = min(STEP_A, sizes[i])
        steps = sizes[i] // n
        index = lambda g, p: p[0] * (heads // n) + begins[i] // n + g
        ins = [queries] + ([q_got[i]] if pair > 1 else []) + [wq_t, wk_t, kv_unit]
        in_specs = [spec((block, n * width), lambda g, p: (0, index(g, p)))]
        if pair > 1:
            in_specs.append(spec((block, n * width), lambda g, p: (0, g)))
        in_specs += [spec((n, half, width), lambda g, p: (index(g, p), 0, 0))] * 2
        in_specs.append(spec((tokens, 2 * width), whole2))
        feat_shape = jax.ShapeDtypeStruct((sizes[i], two, tokens), BF16)
        outs = [jax.ShapeDtypeStruct((sizes[i], tokens, width), BF16)] + [feat_shape] * 4
        outs += [
            jax.ShapeDtypeStruct((sizes[i], pair, width + ROWS, block), F32),
            jax.ShapeDtypeStruct((sizes[i], two, 2 * width), F32),
        ]
        out_specs = [spec((n, tokens, width), per_head3)] + [spec((n, two, tokens), per_head3)] * 4
        out_specs += [
            spec((n, pair, width + ROWS, block), per_head4),
            spec((n, two, 2 * width), per_head3),
        ]
        return pl.pallas_call(
            functools.partial(local_kernel, pair, block, width, half),
            out_shape=outs,
            grid_spec=pltpu.PrefetchScalarGridSpec(
                num_scalar_prefetch=1,
                grid=(steps,),
                in_specs=in_specs,
                out_specs=out_specs,
                scratch_shapes=[
                    pltpu.VMEM((tokens, width), BF16),
                    pltpu.VMEM((tokens, 2 * width), BF16),
                    pltpu.VMEM((width + ROWS, tokens), BF16),
                ],
            ),
            compiler_params=pltpu.CompilerParams(
                dimension_semantics=("arbitrary",), vmem_limit_bytes=VMEM_LIMIT
            ),
            cost_estimate=pl.CostEstimate(
                flops=sizes[i] * tokens * 1_500_000, bytes_accessed=10_000_000, transcendentals=0
            ),
            name="local_part",
        )(pos, *ins)

    def run_global(i, local, kv_all, inv_power):
        n = min(STEP_B, sizes[i])
        steps = sizes[i] // n
        index = lambda g, p: p[0] * (heads // n) + begins[i] // n + g
        ins = [*local, wk_t, teacher]
        in_specs = [spec((n, tokens, width), per_head3)] + [spec((n, two, tokens), per_head3)] * 4
        in_specs += [
            spec((n, pair, width + ROWS, block), per_head4),
            spec((n, two, 2 * width), per_head3),
            spec((n, half, width), lambda g, p: (index(g, p), 0, 0)),
            spec((block, n * width), lambda g, p: (0, index(g, p))),
        ]
        if pair > 1:
            ins.append(t_got[i])
            in_specs.append(spec((block, n * width), lambda g, p: (0, g)))
        ins += [inv_power, kv_all]
        in_specs += [
            spec((1, tokens), whole2),
            spec((units, tokens, 2 * width), lambda g, p: (0, 0, 0)),
        ]
        return pl.pallas_call(
            functools.partial(global_kernel, pair, units, block, width, half),
            out_shape=jax.ShapeDtypeStruct((sizes[i], width, two), F32),
            grid_spec=pltpu.PrefetchScalarGridSpec(
                num_scalar_prefetch=1,
                grid=(steps,),
                in_specs=in_specs,
                out_specs=spec((n, width, two), per_head3),
                scratch_shapes=[
                    pltpu.VMEM((units, tokens, width), BF16),
                    pltpu.VMEM((units, tokens, 2 * width), BF16),
                    pltpu.VMEM((units, 2 * width, tokens), BF16),
                    pltpu.VMEM((max(units - 1, 1), n, two, tokens), F32),
                    pltpu.VMEM((n * two, 2 * width), F32),
                    pltpu.VMEM((2 * width, block), BF16),
                    pltpu.VMEM((2 * width, block), BF16),
                    pltpu.VMEM((n, two, width), F32),
                    pltpu.VMEM((n * two, 2 * width), F32),
                ],
            ),
            compiler_params=pltpu.CompilerParams(
                dimension_semantics=("arbitrary",), vmem_limit_bytes=VMEM_LIMIT
            ),
            cost_estimate=pl.CostEstimate(
                flops=sizes[i] * tokens * 3_000_000, bytes_accessed=10_000_000, transcendentals=0
            ),
            name="global_part",
        )(pos, *ins)

    near = []
    for c, piece in enumerate(pieces):
        slots = {0: piece}
        for i in range(bits):
            bit = 1 << ((i + c) % bits)
            slots[bit] = swap(piece, bit * pair)
        near.append(slots)

    locals_ = [run_local(0)]
    mark = locals_[0][-1]
    flat = [s[1 << i] for s in near for i in range(bits)]
    flat = tie(*flat, mark)[:-1]
    gathered = []
    for c in range(pair):
        got = {1 << i: flat[c * bits + i] for i in range(bits)}
        slots = {0: pieces[c]}
        for i in range(bits):
            bit = 1 << ((i + c) % bits)
            new = {}
            for o in sorted(slots):
                new[o | bit] = got[bit] if o == 0 else swap(slots[o], bit * pair)
            slots.update(new)
        gathered.append(slots)
    power = squares
    for x in tie(*others, mark)[:-1]:
        power = power + x
    inv_power = 1.0 / (power / (head_count * head_axis * width) + 1e-05)
    if pair > 1:
        inv_got = swap(inv_power, 1)
    for i in range(1, count):
        locals_.append(run_local(i))
    mark = locals_[-1][-1]
    if pair > 1:
        inv_got = tie(inv_got, mark)[0]
        inv_power = cat(
            [jnp.where(first, inv_power, inv_got), jnp.where(first, inv_got, inv_power)], 1
        )
    flat = [g[o] for o in range(units) for g in gathered]
    kv_all = cat(tie(*flat, mark)[:-1], 0).reshape(units, tokens, 2 * width)

    share = width // units
    grads, arrived = [], []
    for i in range(count):
        grad = run_global(i, locals_[i], kv_all, inv_power)
        grads.append(grad[:, :share])
        arrived.append(
            [swap(grad[:, o * share : (o + 1) * share], o * pair) for o in range(1, units)]
        )
        mark = grad
    totals = []
    for i in range(count):
        total = grads[i]
        parts = arrived[i]
        if i < count - 1:
            parts = tie(*parts, mark)[:-1]
        for x in parts:
            total = total + x
        totals.append(total)
    total = cat(totals, 0)
    if pair > 1:
        rows = share // pair
        keep = total[:, :rows]
        got = swap(total[:, rows:], 1)
        total = cat([jnp.where(first, keep, got), jnp.where(first, got, keep)], 0)
    return total[..., :half], total[..., half:]


def solution(mesh):
    return jax.shard_map(
        functools.partial(on_device, (mesh.shape["seq"], mesh.shape["head"])),
        mesh=mesh,
        in_specs=(
            P("seq", "head"),
            P("seq", "head"),
            P("seq", "head"),
            P("seq", "head"),
            P("head", None, None),
            P("head", None, None),
        ),
        out_specs=(P("head", "seq", None), P("head", "seq", None)),
        check_vma=False,
    )
```

```python
import functools

import jax
import jax.numpy as jnp
from jax import lax
from jax.experimental import pallas as pl
from jax.experimental.pallas import tpu as pltpu
from jax.sharding import PartitionSpec as P

F32, BF16 = jnp.float32, jnp.bfloat16
LANES = 128
ROWS = 16
STEP_A = 4
STEP_B = 8
PARTS = (1, 1)
VMEM_LIMIT = 60 * 1024 * 1024


def split(x):
    high = x.astype(BF16)
    return high, (x - high.astype(F32)).astype(BF16)


def mm(a, b):
    return jnp.dot(a, b, preferred_element_type=F32)


def mm_nt(a, b):
    return lax.dot_general(a, b, (((1,), (1,)), ((), ())), preferred_element_type=F32)


def cat(parts, axis):
    return jnp.concatenate(parts, axis)


def features(logits):
    up, down = jnp.exp(logits), jnp.exp(-logits)
    up = up * (1.0 / jnp.sum(up, 0, keepdims=True))
    down = down * (1.0 / jnp.sum(down, 0, keepdims=True))
    return cat([up, down], 0)


def features_back(feat, grad):
    half = feat.shape[0] // 2
    prod = feat * grad
    up, down = prod[:half], prod[half:]
    up = up - feat[:half] * jnp.sum(up, 0, keepdims=True)
    down = down - feat[half:] * jnp.sum(down, 0, keepdims=True)
    return up - down


def causal_mask(size):
    row = lax.broadcasted_iota(jnp.int32, (size, size), 0)
    col = lax.broadcasted_iota(jnp.int32, (size, size), 1)
    return row <= col


def with_ones(v):
    return cat([v, jnp.ones_like(v)], 1)


def local_kernel(pair, block, width, half, pos_ref, *refs):
    refs = list(refs)
    q_own = refs.pop(0)
    q_got = refs.pop(0) if pair > 1 else None
    wq, wk, kv = refs[:3]
    q_out, qh_out, ql_out, kh_out, kl_out, num_out, state_out = refs[3:10]
    k_nat, v_aug, v_tr = refs[10:]
    heads = wq.shape[0]
    tokens = pair * block

    @pl.when(pl.program_id(0) == 0)
    def _():
        k_nat[...] = kv[:, :width].astype(BF16)
        v = kv[:, width:]
        v_aug[...] = with_ones(v).astype(BF16)
        v_tr[:width] = v.T.astype(BF16)
        v_tr[width:] = jnp.ones((ROWS, tokens), BF16)

    mask = causal_mask(block)
    each = range(heads)
    spans = [slice(b * block, (b + 1) * block) for b in range(pair)]
    chains = [(h, b) for h in each for b in range(pair)]
    for h in each:
        cols = slice(h * width, (h + 1) * width)
        if pair > 1:
            place = pos_ref[0]
            q_out[h, pl.ds(pl.multiple_of(place * block, block), block)] = q_own[:, cols]
            q_out[h, pl.ds(pl.multiple_of((1 - place) * block, block), block)] = q_got[
                :, cols
            ].astype(BF16)
        else:
            q_out[h] = q_own[:, cols]
    k_logits = mm_nt(wk[...].reshape(heads * half, width), k_nat[...])
    q_logits = [mm_nt(wq[h], q_out[h]) for h in each]
    k_parts = [split(features(k_logits[h * half : (h + 1) * half])) for h in each]
    q_parts = [split(features(q_logits[h])) for h in each]
    for h in each:
        kh_out[h], kl_out[h] = k_parts[h]
        qh_out[h], ql_out[h] = q_parts[h]
    turned = [(k_parts[h][0][:, spans[b]].T, k_parts[h][1][:, spans[b]].T) for h, b in chains]
    scores = []
    for (h, b), (kth, ktl) in zip(chains, turned):
        qh, ql = q_parts[h][0][:, spans[b]], q_parts[h][1][:, spans[b]]
        scores.append(mm(cat([kth, kth, ktl], 1), cat([qh, ql, qh], 0)))
    if pair > 1:
        va = v_aug[:block]
        for h in each:
            kh, kl = k_parts[h]
            state_out[h] = mm(cat([kh[:, :block], kl[:, :block]], 1), cat([va, va], 0))
    else:
        state_out[...] = jnp.zeros_like(state_out)
    masked = [split(jnp.where(mask, x, 0.0)) for x in scores]
    for (h, b), (sh, sl) in zip(chains, masked):
        vt = v_tr[:, spans[b]]
        num_out[h, b] = mm(cat([vt, vt], 1), cat([sh, sl], 0))


def global_kernel(pair, units, block, width, half, pos_ref, *refs):
    refs = list(refs)
    q, qh_in, ql_in, kh_in, kl_in, num_in, state_in, wk, t_own = refs[:9]
    refs = refs[9:]
    t_got = refs.pop(0) if pair > 1 else None
    inv_power = refs.pop(0)
    kv, refs = refs[: units * pair], refs[units * pair :]
    outs, refs = refs[:units], refs[units:]
    k_nat, v_aug, feat_old, state, grad_k, gsum, turn = refs
    two = 2 * half
    heads = wk.shape[0]
    tokens = pair * block
    place, unit = pos_ref[0], pos_ref[1]

    @pl.when(pl.program_id(0) == 0)
    def _():
        for o in range(units):
            for c in range(pair):
                at = slice(c * block, (c + 1) * block)
                k_nat[o, at] = kv[o * pair + c][:, :width].astype(BF16)
                v_aug[o, at] = with_ones(kv[o * pair + c][:, width:]).astype(BF16)

    wk_all = wk[...].reshape(heads * half, width)
    state[...] = jnp.zeros_like(state)

    def ahead(u, carry):
        o = unit ^ u
        logits = mm_nt(wk_all, k_nat[o])
        highs, lows = [], []
        feats = [features(logits[h * half : (h + 1) * half]) for h in range(heads)]
        for h, feat in enumerate(feats):
            feat_old[u, h] = feat
            fh, fl = split(feat)
            highs.append(fh)
            lows.append(fl)
        va = v_aug[o]
        state[...] += mm(cat([cat(highs, 0), cat(lows, 0)], 1), cat([va, va], 0))
        return carry

    lax.fori_loop(0, unit, ahead, 0)

    mask = causal_mask(block)
    each = range(heads)
    spans = [slice(b * block, (b + 1) * block) for b in range(pair)]
    chains = [(h, b) for h in each for b in range(pair)]

    def three(x, y, axis_x, axis_y):
        return cat([x[0], x[0], x[1]], axis_x), cat([y[0], y[1], y[0]], axis_y)

    def feat_of(high, low):
        return high.astype(F32) + low.astype(F32)

    totals = []
    for h, b in chains:
        x = state[h * two : (h + 1) * two]
        totals.append(x + state_in[h] if b == 1 else x)
    states = [split(x) for x in totals]
    turned = [
        split(cat([x[:, :width].T, x[:, width : width + LANES].T[:ROWS]], 0)) for x in totals
    ]
    qs = [(qh_in[h, :, spans[b]], ql_in[h, :, spans[b]]) for h, b in chains]
    ks = [(kh_in[h, :, spans[b]], kl_in[h, :, spans[b]]) for h, b in chains]
    numers = [
        num_in[h, b] + mm(*three(t, q_, 1, 0)) for (h, b), t, q_ in zip(chains, turned, qs)
    ]
    targets = []
    for h, b in chains:
        own_t = t_own[:, h * width : (h + 1) * width].astype(F32)
        if pair > 1:
            own_t = jnp.where(place == b, own_t, t_got[:, h * width : (h + 1) * width])
        targets.append(own_t.T)
    top = lax.broadcasted_iota(jnp.int32, (ROWS, block), 0) == 0
    small, full = [], []
    for (h, b), numer, target in zip(chains, numers, targets):
        inv = 1.0 / numer[width : width + 1]
        student = numer[:width] * inv
        grad_out = (student - target) * inv_power[0:1, spans[b]]
        gden = -jnp.sum(grad_out * student, 0, keepdims=True) * inv
        gh, gl = split(grad_out * inv)
        dh, dl = split(jnp.where(top, gden, 0.0))
        pad = jnp.zeros((width - ROWS, block), BF16)
        small.append((cat([gh, dh], 0), cat([gl, dl], 0)))
        full.append((cat([gh, dh, pad], 0), cat([gl, dl, pad], 0)))
    backs = []
    for (h, b), g in zip(chains, full):
        va = v_aug[0, spans[b]]
        backs.append(mm(cat([va, va], 1), cat([g[0], g[1]], 0)))
    grad_q = [mm(*three(st, g, 1, 0)) for st, g in zip(states, full)]
    sums = [mm_nt(*three(g, q_, 1, 1)) for g, q_ in zip(small, qs)]
    backs = [split(jnp.where(mask, x, 0.0)) for x in backs]
    grad_q = [g + mm(*three(k, x, 1, 0)) for g, k, x in zip(grad_q, ks, backs)]
    key_grads = [mm_nt(*three(q_, x, 1, 1)) for q_, x in zip(qs, backs)]

    def widen(x):
        return cat([x, jnp.zeros((width - ROWS, width), F32)], 0).T

    wide = [widen(x) for x in sums]
    for h in each:
        later = None
        for b in reversed(range(pair)):
            n = h * pair + b
            if later is not None:
                ph, plow = split(later)
                va = v_aug[0, spans[b]]
                key_grads[n] = key_grads[n] + mm_nt(cat([ph, plow], 1), cat([va, va], 1))
            later = wide[n] if later is None else later + wide[n]
        gsum[h * two : (h + 1) * two] = later
    q_logit = [split(features_back(feat_of(*q_), g)) for q_, g in zip(qs, grad_q)]
    k_logit = [split(features_back(feat_of(*k), g)) for k, g in zip(ks, key_grads)]
    for h in each:
        rows = range(h * pair, (h + 1) * pair)
        left = cat([x for n in rows for x in q_logit[n]], 1)
        right = cat([q[h, spans[b]] for b in range(pair) for _ in range(2)], 0)
        grad_k[h, :half] = mm(left, right)
    for b in range(pair):
        highs = cat([k_logit[h * pair + b][0] for h in each], 0)
        lows = cat([k_logit[h * pair + b][1] for h in each], 0)
        k_blk = k_nat[0, spans[b]]
        add = mm(cat([highs, lows], 1), cat([k_blk, k_blk], 0))
        for h in each:
            if b == 0:
                grad_k[h, half:] = add[h * half : (h + 1) * half]
            else:
                grad_k[h, half:] += add[h * half : (h + 1) * half]

    gsh, gsl = split(gsum[...])
    both = cat([gsh, gsl], 1)

    def behind(u, carry):
        o = unit ^ u
        va = v_aug[o]
        gk = mm_nt(both, cat([va, va], 1))
        highs, lows = [], []
        for h in range(heads):
            lh, ll = split(
                features_back(feat_old[u, h], gk[h * 2 * half : (h + 1) * 2 * half])
            )
            highs.append(lh)
            lows.append(ll)
        k_blk = k_nat[o]
        add = mm(cat([cat(highs, 0), cat(lows, 0)], 1), cat([k_blk, k_blk], 0))
        for h in range(heads):
            grad_k[h, half:] += add[h * half : (h + 1) * half]
        return carry

    lax.fori_loop(0, unit, behind, 0)

    share = width // (units * pair)
    for h in each:
        turn[h] = grad_k[h].T
    for h in each:
        for o in range(units):
            for r in range(pair):
                start = pl.multiple_of(((unit ^ o) * pair + (place ^ r)) * share, share)
                outs[o][h, r * share : (r + 1) * share] = turn[h, pl.ds(start, share)]


def on_device(axis_sizes, queries, keys, values, teacher, map_q, map_k):
    seq_count, head_axis = axis_sizes
    head_count, width, half = map_q.shape
    block = queries.shape[0]
    shared = keys.shape[1] // width
    pair = 2 if shared == 2 and seq_count % 2 == 0 else 1
    units = seq_count // pair
    heads = head_count // pair
    tokens = pair * block
    bits = units.bit_length() - 1
    own = lax.axis_index("seq")
    place, unit = own % pair, own // pair
    pos = jnp.stack([place, unit]).astype(jnp.int32)
    columns = heads * width

    def swap(x, bit):
        return lax.ppermute(x, "seq", [(i, i ^ bit) for i in range(seq_count)])

    def mine(x, size, index):
        return lax.dynamic_slice_in_dim(x, index * size, size, 1)

    def tie(*values):
        return lax.optimization_barrier(values)

    kv = cat([mine(keys, width, place), mine(values, width, place)], 1).astype(F32)
    count = len(PARTS)
    sizes = [heads * n // sum(PARTS) for n in PARTS]
    begins = [sum(sizes[:i]) for i in range(count)]
    first = place == 0
    q_got, t_got = [None] * count, [None] * count
    if pair > 1:
        other = 1 - place
        kv_away = cat([mine(keys, width, other), mine(values, width, other)], 1).astype(F32)
        q_src, kv_away = tie(queries, kv_away)
        kv_got = swap(kv_away, 1)

        def away(source, i):
            start = other * columns + begins[i] * width
            return lax.dynamic_slice_in_dim(source, start, sizes[i] * width, 1).astype(F32)

        q_away = [away(q_src, i) for i in range(count)]
        q_got = [swap(x, 1) for x in q_away]
        t_src, q_last = tie(teacher, q_away[-1])
        t_got = [swap(away(t_src, i), 1) for i in range(count)]
        pieces = [jnp.where(first, kv, kv_got), jnp.where(first, kv_got, kv)]
    else:
        pieces = [kv]
    kv_unit = cat(pieces, 0)

    squares = jnp.sum(jnp.square(teacher.astype(F32)), axis=1)[None]
    others = [
        lax.ppermute(squares, "head", [(i, (i + s) % head_axis) for i in range(head_axis)])
        for s in range(1, head_axis)
    ]

    wq_t, wk_t = jnp.swapaxes(map_q, 1, 2), jnp.swapaxes(map_k, 1, 2)
    two = 2 * half
    whole2 = lambda g, p: (0, 0)
    per_head3 = lambda g, p: (g, 0, 0)
    per_head4 = lambda g, p: (g, 0, 0, 0)
    spec = pl.BlockSpec

    def run_local(i):
        n = min(STEP_A, sizes[i])
        steps = sizes[i] // n
        index = lambda g, p: p[0] * (heads // n) + begins[i] // n + g
        ins = [queries] + ([q_got[i]] if pair > 1 else []) + [wq_t, wk_t, kv_unit]
        in_specs = [spec((block, n * width), lambda g, p: (0, index(g, p)))]
        if pair > 1:
            in_specs.append(spec((block, n * width), lambda g, p: (0, g)))
        in_specs += [spec((n, half, width), lambda g, p: (index(g, p), 0, 0))] * 2
        in_specs.append(spec((tokens, 2 * width), whole2))
        feat_shape = jax.ShapeDtypeStruct((sizes[i], two, tokens), BF16)
        outs = [jax.ShapeDtypeStruct((sizes[i], tokens, width), BF16)] + [feat_shape] * 4
        outs += [
            jax.ShapeDtypeStruct((sizes[i], pair, width + ROWS, block), F32),
            jax.ShapeDtypeStruct((sizes[i], two, 2 * width), F32),
        ]
        out_specs = [spec((n, tokens, width), per_head3)] + [spec((n, two, tokens), per_head3)] * 4
        out_specs += [
            spec((n, pair, width + ROWS, block), per_head4),
            spec((n, two, 2 * width), per_head3),
        ]
        return pl.pallas_call(
            functools.partial(local_kernel, pair, block, width, half),
            out_shape=outs,
            grid_spec=pltpu.PrefetchScalarGridSpec(
                num_scalar_prefetch=1,
                grid=(steps,),
                in_specs=in_specs,
                out_specs=out_specs,
                scratch_shapes=[
                    pltpu.VMEM((tokens, width), BF16),
                    pltpu.VMEM((tokens, 2 * width), BF16),
                    pltpu.VMEM((width + ROWS, tokens), BF16),
                ],
            ),
            compiler_params=pltpu.CompilerParams(
                dimension_semantics=("arbitrary",), vmem_limit_bytes=VMEM_LIMIT
            ),
            cost_estimate=pl.CostEstimate(
                flops=sizes[i] * tokens * 1_500_000, bytes_accessed=10_000_000, transcendentals=0
            ),
            name="local_part",
        )(pos, *ins)

    def run_global(i, local, kv_all, inv_power):
        n = max(d for d in range(1, STEP_B + 1) if sizes[i] % d == 0 and begins[i] % d == 0)
        steps = sizes[i] // n
        index = lambda g, p: p[0] * (heads // n) + begins[i] // n + g
        ins = [*local, wk_t, teacher]
        in_specs = [spec((n, tokens, width), per_head3)] + [spec((n, two, tokens), per_head3)] * 4
        in_specs += [
            spec((n, pair, width + ROWS, block), per_head4),
            spec((n, two, 2 * width), per_head3),
            spec((n, half, width), lambda g, p: (index(g, p), 0, 0)),
            spec((block, n * width), lambda g, p: (0, index(g, p))),
        ]
        if pair > 1:
            ins.append(t_got[i])
            in_specs.append(spec((block, n * width), lambda g, p: (0, g)))
        ins += [inv_power, *kv_all]
        in_specs.append(spec((1, tokens), whole2))
        in_specs += [spec((block, 2 * width), whole2)] * len(kv_all)
        return pl.pallas_call(
            functools.partial(global_kernel, pair, units, block, width, half),
            out_shape=[jax.ShapeDtypeStruct((sizes[i], width // units, two), F32)] * units,
            grid_spec=pltpu.PrefetchScalarGridSpec(
                num_scalar_prefetch=1,
                grid=(steps,),
                in_specs=in_specs,
                out_specs=[spec((n, width // units, two), per_head3)] * units,
                scratch_shapes=[
                    pltpu.VMEM((units, tokens, width), BF16),
                    pltpu.VMEM((units, tokens, 2 * width), BF16),
                    pltpu.VMEM((max(units - 1, 1), n, two, tokens), F32),
                    pltpu.VMEM((n * two, 2 * width), F32),
                    pltpu.VMEM((n, two, width), F32),
                    pltpu.VMEM((n * two, 2 * width), F32),
                    pltpu.VMEM((n, width, two), F32),
                ],
            ),
            compiler_params=pltpu.CompilerParams(
                dimension_semantics=("arbitrary",), vmem_limit_bytes=VMEM_LIMIT
            ),
            cost_estimate=pl.CostEstimate(
                flops=sizes[i] * tokens * 3_000_000, bytes_accessed=10_000_000, transcendentals=0
            ),
            name="global_part",
        )(pos, *ins)

    near = []
    for c, piece in enumerate(pieces):
        slots = {0: piece}
        for i in range(bits):
            bit = 1 << ((i + c) % bits)
            slots[bit] = swap(piece, bit * pair)
        near.append(slots)

    locals_ = [run_local(0)]
    mark = locals_[0][-1]
    flat = [s[1 << i] for s in near for i in range(bits)]
    flat = tie(*flat, mark)[:-1]
    gathered = []
    for c in range(pair):
        got = {1 << i: flat[c * bits + i] for i in range(bits)}
        slots = {0: pieces[c]}
        for i in range(bits):
            bit = 1 << ((i + c) % bits)
            new = {}
            for o in sorted(slots):
                new[o | bit] = got[bit] if o == 0 else swap(slots[o], bit * pair)
            slots.update(new)
        gathered.append(slots)
    power = squares
    for x in tie(*others, mark)[:-1]:
        power = power + x
    inv_power = 1.0 / (power / (head_count * head_axis * width) + 1e-05)
    if pair > 1:
        inv_got = swap(inv_power, 1)
    for i in range(1, count):
        locals_.append(run_local(i))
    mark = locals_[-1][-1]
    if pair > 1:
        inv_got = tie(inv_got, mark)[0]
        inv_power = cat(
            [jnp.where(first, inv_power, inv_got), jnp.where(first, inv_got, inv_power)], 1
        )
    flat = [g[o] for o in range(units) for g in gathered]
    kv_all = tie(*flat, mark)[:-1]

    share = width // units
    grads, arrived = [None] * count, [None] * count
    order = sorted(range(count), key=lambda i: -sizes[i])
    for i in order:
        grad = run_global(i, locals_[i], kv_all, inv_power)
        grads[i] = grad[0]
        arrived[i] = [swap(grad[o], o * pair) for o in range(1, units)]
        inv_power, mark = tie(inv_power, grad[0])
    totals = []
    for i in range(count):
        total = grads[i]
        parts = arrived[i]
        if i != order[-1]:
            parts = tie(*parts, mark)[:-1]
        for x in parts:
            total = total + x
        totals.append(total)
    total = cat(totals, 0)
    if pair > 1:
        rows = share // pair
        keep = total[:, :rows]
        got = swap(total[:, rows:], 1)
        total = cat([jnp.where(first, keep, got), jnp.where(first, got, keep)], 0)
    return total[..., :half], total[..., half:]


def solution(mesh):
    return jax.shard_map(
        functools.partial(on_device, (mesh.shape["seq"], mesh.shape["head"])),
        mesh=mesh,
        in_specs=(
            P("seq", "head"),
            P("seq", "head"),
            P("seq", "head"),
            P("seq", "head"),
            P("head", None, None),
            P("head", None, None),
        ),
        out_specs=(P("head", "seq", None), P("head", "seq", None)),
        check_vma=False,
    )
```
